32 devices in a mesh: dp: 4 (over z), cp: 2 (over x), tp: 4 (over y, core).
Axes of the slice: x: 2, y: 2, z: 4, core: 2. Of those that a mesh axis runs over, the one named last changes fastest.
Arguments:
- tokens: bfloat16 [4, 1024, 2048], P('dp', 'cp'), may hold values from -6 to 6
- source_ids: int32 [4, 1024], P('dp', 'cp'), may hold values from 0 to 3, never falling along the last dimension, each value on 1 to 512 neighbouring positions
- pad_mask: int32 [4, 1024], P('dp', 'cp'), may hold values from 0 to 1, as said below
- cotangent: bfloat16 [4, 1024, 2048], P('dp', 'cp'), may hold values from -6 to 6
- w_query: bfloat16 [2048, 2048], P(None, 'tp'), may hold values from -0.125 to 0.125
- w_key: bfloat16 [2048, 2048], P(None, 'tp'), may hold values from -0.125 to 0.125
- w_value: bfloat16 [2048, 2048], P(None, 'tp'), may hold values from -0.125 to 0.125
- w_out: bfloat16 [2048, 2048], P('tp'), may hold values from -0.125 to 0.125
- w_gate: bfloat16 [2048, 8192], P(None, 'tp'), may hold values from -0.125 to 0.125
- w_up: bfloat16 [2048, 8192], P(None, 'tp'), may hold values from -0.125 to 0.125
- w_down: bfloat16 [8192, 2048], P('tp'), may hold values from -0.0625 to 0.0625
- gain_query: float32 [2048], P('tp'), may hold values from 0.1 to 1.9
- gain_key: float32 [2048], P('tp'), may hold values from 0.1 to 1.9
- gain_attn: float32 [2048], replicated, may hold values from 0.1 to 1.9
- gain_mlp: float32 [2048], replicated, may hold values from 0.1 to 1.9
Outputs:
- output: bfloat16 [4, 1024, 2048], P('dp', 'cp')
- grad_tokens: bfloat16 [4, 1024, 2048], P('dp', 'cp')
- grad_w_query: float32 [2048, 2048], P(('dp', 'cp'), 'tp')
- grad_w_key: float32 [2048, 2048], P(('dp', 'cp'), 'tp')
- grad_w_value: float32 [2048, 2048], P(('dp', 'cp'), 'tp')
- grad_w_out: float32 [2048, 2048], P('tp', ('dp', 'cp'))
- grad_w_gate: float32 [2048, 8192], P(('dp', 'cp'), 'tp')
- grad_w_up: float32 [2048, 8192], P(('dp', 'cp'), 'tp')
- grad_w_down: float32 [8192, 2048], P('tp', ('dp', 'cp'))
- grad_gain_query: float32 [2048], P('tp')
- grad_gain_key: float32 [2048], P('tp')
- grad_gain_attn: float32 [2048], replicated
- grad_gain_mlp: float32 [2048], replicated
The draws below stay inside these ranges and needn't reach their ends.
Inputs may be any that keep to these rules, and one draw needn't show every extreme that they name: `pad_mask`: in each sequence the ones come first and cover 1024 // 2 or more positions; the last position is always 0. `source_ids`: never falls along a sequence; each value is one run of 1 to 512 positions, and one run is exactly 512 long.
All inputs are finite; a program needn't handle non-finite values.
Results may differ from the reference program's by a relative error of at most 0.017.
Values may be sent and summed in bfloat16 or wider, within the bound.
A program may use at most 256 MiB of HBM per device.

```python
import math
import jax
import jax.numpy as jnp
import numpy as np
from jax import lax

D = 2048
HEADS = 16
HEAD_DIM = 128
FF = 8192
LENGTH = 1024
SEQ_ALL = 4


def draw_pad_mask(key, part):
    keep_count = jax.random.randint(key, (SEQ_ALL, 1), LENGTH // 2, LENGTH)
    places = jnp.arange(LENGTH, dtype=jnp.int32)[None, :]
    return (places < keep_count).astype(jnp.int32)


def steps_of(stream_key, shape, cuts, least, high):
    def one(dim, shards_of):
        steps = jax.random.uniform(jax.random.fold_in(jax.random.fold_in(stream_key, 6), dim), (shards_of,), jnp.float32, least / len(cuts), high / len(cuts))
        return jnp.repeat(jnp.exp(steps), shape[dim] // shards_of).reshape((-1,) + (1,) * (len(shape) - dim - 1))

    gain = one(*cuts[0])
    for cut in cuts[1:]:
        gain = gain * one(*cut)
    return gain


def length_profile(number_of, total, most, skew):
    loads = [(1 << 20) // math.isqrt(grade ** skew) + 1 for grade in range(2, number_of + 1)]
    surplus, holding = total - most - (number_of - 1), [1] * (number_of - 1)
    while surplus > 0:
        candidates = [i for i in range(number_of - 1) if holding[i] < most]
        mass, remaining = sum([loads[i] for i in candidates]), surplus
        for i in candidates:
            addition = min(most - holding[i], max(1, remaining * loads[i] // mass), surplus)
            holding[i] = holding[i] + addition
            surplus = surplus - addition
    return np.array([most] + holding)


def uneven_parts(own_key, number_of, total, limit, lean):
    if number_of == 2:
        one = jax.random.randint(own_key, (), max(1, total - limit), min(limit, total - 1) + 1)
        return jnp.stack([one, total - one])
    sizes = jnp.asarray(length_profile(number_of, total, limit, lean), jnp.int32)
    couples = (number_of - 1) // 2
    giver, sink = sizes[1:1 + 2 * couples:2], sizes[2:2 + 2 * couples:2]
    margin = jnp.minimum(giver - 1, limit - sink)
    shifted = jax.random.randint(jax.random.fold_in(own_key, 1), (couples,), 0, 1 << 20) % (margin + 1)
    sizes = sizes.at[1:1 + 2 * couples:2].set(giver - shifted).at[2:2 + 2 * couples:2].set(sink + shifted)
    return sizes[jax.random.permutation(jax.random.fold_in(own_key, 2), number_of)]


def gaussian(stream_key, extent, width, limit, pieces=(), held_as=jnp.bfloat16):
    values = jax.random.normal(stream_key, extent, jnp.float32) * width
    if len(pieces) > 0:
        values = steps_of(stream_key, extent, pieces, -0.22, 0.18) * values
    return jnp.clip(values, min=-limit, max=limit).astype(held_as)


def setup_inputs(seed: int = 0) -> dict:
    streams_of = jax.random.split(jax.random.key(seed), 16)
    return {
        "tokens": gaussian(streams_of[0], (SEQ_ALL, LENGTH, D), 1.0, 6.0, ((0, 4), (1, 2))),
        "source_ids": jax.vmap(lambda own: jnp.searchsorted(jnp.cumsum(uneven_parts(own, 4, LENGTH, LENGTH // 2, 2)), jnp.arange(LENGTH), side="right"))(jax.random.split(streams_of[1], SEQ_ALL)).reshape((SEQ_ALL, LENGTH)).astype(jnp.int32),
        "pad_mask": draw_pad_mask(jax.random.fold_in(streams_of[15], 71), 0),
        "cotangent": gaussian(streams_of[3], (SEQ_ALL, LENGTH, D), 1.0, 6.0, ((0, 4), (1, 2))),
        "w_query": gaussian(streams_of[4], (D, D), D ** -0.5, 0.125, ((1, 4),)),
        "w_key": gaussian(streams_of[5], (D, D), D ** -0.5, 0.125, ((1, 4),)),
        "w_value": gaussian(streams_of[6], (D, D), D ** -0.5, 0.125, ((1, 4),)),
        "w_out": gaussian(streams_of[7], (D, D), D ** -0.5, 0.125, ((0, 4),)),
        "w_gate": gaussian(streams_of[8], (D, FF), D ** -0.5, 0.125, ((1, 4),)),
        "w_up": gaussian(streams_of[9], (D, FF), D ** -0.5, 0.125, ((1, 4),)),
        "w_down": gaussian(streams_of[10], (FF, D), FF ** -0.5, 0.0625, ((0, 4),)),
        "gain_query": jnp.clip(1.0 + 0.18 * jax.random.normal(streams_of[11], (D,), jnp.float32), 0.1, 1.9),
        "gain_key": jnp.clip(1.0 + 0.18 * jax.random.normal(streams_of[12], (D,), jnp.float32), 0.1, 1.9),
        "gain_attn": jnp.clip(1.0 + 0.18 * jax.random.normal(streams_of[13], (D,), jnp.float32), 0.1, 1.9),
        "gain_mlp": jnp.clip(1.0 + 0.18 * jax.random.normal(streams_of[14], (D,), jnp.float32), 0.1, 1.9),
    }


EPS = 1e-06
ROPE_BASE = 500000.0
NEG = -1e+30

@jax.custom_vjp
def low(v):
    return lax.optimization_barrier(v.astype(jnp.bfloat16)).astype(jnp.float32)

@jax.custom_vjp
def low_back(v):
    return v

def low_keep(v):
    return (low(v), None)

def low_pass(kept, grad):
    return (grad,)

def back_keep(v):
    return (v, None)

def back_low(kept, grad):
    return (low(grad),)
low.defvjp(low_keep, low_pass)
low_back.defvjp(back_keep, back_low)

def matmul_high(left, right):
    return jnp.dot(left, right, precision=lax.Precision.HIGHEST)

def norm_apply(values, gain_vec):
    return values * lax.rsqrt(lax.optimization_barrier(jnp.mean(values * values, -1, keepdims=True)) + EPS) * gain_vec

def rope_turn(values, places, direction):
    half_dim = values.shape[-1] // 2
    freqs = ROPE_BASE ** (-(jnp.arange(half_dim, dtype=jnp.float32) * 2.0 / values.shape[-1]))
    angles = places[:, None] * freqs[None, :]
    cosine = jnp.concatenate([jnp.cos(angles), jnp.cos(angles)], -1)[:, None, :]
    sine = jnp.concatenate([jnp.sin(angles), jnp.sin(angles)], -1)[:, None, :]
    turned = jnp.concatenate([-values[..., half_dim:], values[..., :half_dim]], -1)
    return values * cosine + direction * turned * sine

def layer(inputs, segment, valid, params):
    w_query, w_key, w_value, w_out, w_gate, w_up, w_down, gain_query, gain_key, gain_attn, gain_mlp = params
    length = inputs.shape[0]
    places = jnp.arange(length, dtype=jnp.float32)
    query_raw = low_back(matmul_high(inputs, w_query))
    key_raw = low_back(matmul_high(inputs, w_key))
    value_low = low(low_back(matmul_high(inputs, w_value)))
    query_rot = low(rope_turn(norm_apply(query_raw, gain_query).reshape(length, HEADS, HEAD_DIM), places, 1.0))
    key_rot = low(rope_turn(norm_apply(key_raw, gain_key).reshape(length, HEADS, HEAD_DIM), places, 1.0))
    value_heads = value_low.reshape(length, HEADS, HEAD_DIM)
    block_rows = min(512, length)
    key_index = jnp.arange(length, dtype=jnp.int32)
    key_code = jnp.where(valid > 0, segment, -1)

    def attend(start):
        query_block = lax.dynamic_slice_in_dim(query_rot, start, block_rows, 0)
        query_segment = lax.dynamic_slice_in_dim(segment, start, block_rows, 0)
        query_index = start + jnp.arange(block_rows, dtype=jnp.int32)
        scores = jnp.einsum('qhd,khd->hqk', query_block, key_rot, precision=lax.Precision.HIGHEST) * HEAD_DIM ** (-0.5)
        scores = low_back(scores)
        allowed = (key_index[None, :] <= query_index[:, None]) & ((key_code[None, :] == query_segment[:, None]) | (key_index[None, :] == query_index[:, None]))
        scores = jnp.where(allowed[None], scores, NEG)
        largest = lax.optimization_barrier(jnp.max(scores, -1, keepdims=True))
        raw_weights = jnp.exp(scores - largest)
        probs = low(raw_weights / lax.optimization_barrier(jnp.sum(raw_weights, -1, keepdims=True)))
        return jnp.einsum('hqk,khd->qhd', probs, value_heads, precision=lax.Precision.HIGHEST)
    starts = jnp.arange(length // block_rows, dtype=jnp.int32) * block_rows
    attended = lax.map(jax.checkpoint(attend), starts).reshape(length, D)
    attn_low = low(low_back(attended))
    branch_a = low_back(matmul_high(attn_low, w_out))
    hidden = inputs + norm_apply(branch_a, gain_attn)
    hidden_low = low(hidden)
    gate = low_back(matmul_high(hidden_low, w_gate))
    up_part = low_back(matmul_high(hidden_low, w_up))
    act_low = low(jax.nn.silu(gate) * up_part)
    branch_m = low_back(matmul_high(act_low, w_down))
    return hidden + norm_apply(branch_m, gain_mlp)

def reference(tokens, source_ids, pad_mask, cotangent, w_query, w_key, w_value, w_out, w_gate, w_up, w_down, gain_query, gain_key, gain_attn, gain_mlp):
    params = (w_query.astype(jnp.float32), w_key.astype(jnp.float32), w_value.astype(jnp.float32), w_out.astype(jnp.float32), w_gate.astype(jnp.float32), w_up.astype(jnp.float32), w_down.astype(jnp.float32), gain_query.astype(jnp.float32), gain_key.astype(jnp.float32), gain_attn.astype(jnp.float32), gain_mlp.astype(jnp.float32))

    def one_seq(carry, seq_items):
        inputs, segment, valid, seq_grad = seq_items

        def apply_layer(inputs_f, params_f):
            return layer(inputs_f, segment, valid, params_f)
        result, pullback = jax.vjp(apply_layer, inputs.astype(jnp.float32), params)
        grad_inputs, grad_params = pullback(seq_grad.astype(jnp.float32))
        carry = jax.tree.map(lambda left, right: left + right, carry, grad_params)
        return (carry, (result.astype(jnp.bfloat16), grad_inputs.astype(jnp.bfloat16)))
    start_grads = jax.tree.map(jnp.zeros_like, params)
    grads, (output, grad_tokens) = lax.scan(one_seq, start_grads, (tokens, source_ids, pad_mask, cotangent))
    return (output, grad_tokens, grads[0], grads[1], grads[2], grads[3], grads[4], grads[5], grads[6], grads[7], grads[8], grads[9], grads[10])
```

```python
import jax
import jax.numpy as jnp
from jax import lax
from jax.sharding import PartitionSpec as P

HEAD_DIM = 128


EPS = 1e-06
ROPE_BASE = 500000.0
NEG = -1e30


def project(left, right):
    return jnp.dot(left, right, preferred_element_type=jnp.float32)


def project_back(left, right):
    return lax.dot_general(
        left, right, (((1,), (1,)), ((), ())), preferred_element_type=jnp.float32
    )


def weight_grad(left, right):
    return lax.dot_general(
        left, right, (((0,), (0,)), ((), ())), preferred_element_type=jnp.float32
    )


def rope_turn(values, places, direction):
    half_dim = values.shape[-1] // 2
    freqs = ROPE_BASE ** (-(jnp.arange(half_dim, dtype=jnp.float32) * 2.0 / values.shape[-1]))
    angles = places[:, None] * freqs[None, :]
    cosine = jnp.concatenate([jnp.cos(angles), jnp.cos(angles)], -1)[:, None, :]
    sine = jnp.concatenate([jnp.sin(angles), jnp.sin(angles)], -1)[:, None, :]
    turned = jnp.concatenate([-values[..., half_dim:], values[..., :half_dim]], -1)
    return values * cosine + direction * turned * sine


CHUNKS = 2


def swap(values, axis, bit):
    size = lax.axis_size(axis)
    return lax.ppermute(values, axis, [(i, i ^ bit) for i in range(size)])


def narrow(values):
    return lax.reduce_precision(values, 8, 7).astype(jnp.bfloat16)


def wide(values):
    return values.astype(jnp.float32)


def local_order(values, core):
    rows = values.shape[0]
    parts = values.reshape(CHUNKS, 2, rows // (2 * CHUNKS), values.shape[1])
    flipped = jnp.concatenate([parts[:, 1:], parts[:, :1]], 1)
    return jnp.where(core == 0, parts, flipped).reshape(values.shape)


def tp_sum(partial):
    half = partial.shape[0] // 2
    arrived = swap(narrow(partial[half:]), "tp", 1)
    chip_sum = narrow(partial[:half] + wide(arrived))
    total = narrow(wide(chip_sum) + wide(swap(chip_sum, "tp", 2)))
    return jnp.concatenate([total, swap(total, "tp", 1)], 0)


def tp_sum_small(values):
    return (values + swap(values, "tp", 1)) + (swap(values, "tp", 2) + swap(values, "tp", 3))


def relative_pieces(values, place):
    width = values.shape[1] // 8
    pieces = [values[:, i * width : (i + 1) * width] for i in range(8)]
    for bit in (1, 2, 4):
        taken = (place & bit) > 0
        pieces = [jnp.where(taken, pieces[i ^ bit], pieces[i]) for i in range(8)]
    return pieces


class Split:
    def __init__(self, values, place, fast):
        self.fast = fast
        self.values = values
        if not fast:
            return
        pieces = relative_pieces(values, place)
        there = swap(jnp.concatenate([pieces[3], pieces[7], pieces[1], pieces[5]], 1), "cp", 1)
        half = there.shape[1] // 2
        self.sent = (jnp.concatenate([pieces[2], pieces[6]], 1), there[:, :half])
        self.kept = (jnp.concatenate([pieces[0], pieces[4]], 1), there[:, half:])


def split_grad(split, values, there, dim):
    if not split.fast:
        partial = weight_grad(split.values, values) if dim == 0 else weight_grad(values, split.values)
        return wide(
            lax.psum_scatter(narrow(partial), ("dp", "cp"), scatter_dimension=dim, tiled=True)
        )

    def both(pair):
        if dim == 0:
            return weight_grad(pair[0], values) + weight_grad(pair[1], there)
        return weight_grad(values, pair[0]) + weight_grad(there, pair[1])

    outgoing = narrow(both(split.sent))
    kept = both(split.kept)
    block = kept.shape[dim] // 2
    arrived = swap(outgoing, "dp", 1)
    onward = lax.slice_in_dim(kept, block, 2 * block, axis=dim) + wide(
        lax.slice_in_dim(arrived, block, 2 * block, axis=dim)
    )
    own = lax.slice_in_dim(kept, 0, block, axis=dim) + wide(
        lax.slice_in_dim(arrived, 0, block, axis=dim)
    )
    return own + wide(swap(narrow(onward), "dp", 2))


def shards(
    tokens,
    source_ids,
    pad_mask,
    cotangent,
    w_query,
    w_key,
    w_value,
    w_out,
    w_gate,
    w_up,
    w_down,
    gain_query,
    gain_key,
    gain_attn,
    gain_mlp,
):
    dp_size, cp_size, tp_size = (lax.axis_size(name) for name in ("dp", "cp", "tp"))
    assert tp_size == 4
    fast = dp_size == 4 and cp_size == 2
    seq_count, shard_rows, model_width = tokens.shape
    local_width = w_query.shape[1]
    head_count = local_width // HEAD_DIM
    row_count = seq_count * shard_rows
    chunk_rows = row_count // CHUNKS
    own_rows = chunk_rows // 2
    score_scale = HEAD_DIM ** (-0.5)
    core = lax.axis_index("tp") % 2
    cp_index = lax.axis_index("cp")
    place = lax.axis_index("dp") * cp_size + cp_index

    def token_sum(values):
        if not fast:
            return lax.psum(values, ("dp", "cp"))
        values = values + swap(values, "cp", 1)
        values = values + swap(values, "dp", 1)
        return values + swap(values, "dp", 2)

    def exchange(values):
        return swap(values, "cp", 1) if fast else None

    tokens_low = tokens.reshape(row_count, model_width)
    query_index = cp_index * shard_rows + jnp.arange(shard_rows, dtype=jnp.int32)
    places = jnp.tile(query_index.astype(jnp.float32), seq_count)
    key_code = jnp.where(pad_mask > 0, source_ids, -1)
    if fast:
        all_codes = jnp.concatenate([key_code, swap(key_code, "cp", 1)], 1)
        key_index = jnp.concatenate([query_index, (1 - cp_index) * shard_rows + jnp.arange(shard_rows, dtype=jnp.int32)])
    else:
        all_codes = lax.all_gather(key_code, "cp", axis=1, tiled=True)
        key_index = jnp.arange(cp_size * shard_rows, dtype=jnp.int32)

    def whole_sequence(values):
        if fast:
            return jnp.concatenate([values, swap(values, "cp", 1)], 1)
        return lax.all_gather(values, "cp", axis=1, tiled=True)

    def back_to_block(values):
        if fast:
            return values[:, :shard_rows] + wide(swap(narrow(values[:, shard_rows:]), "cp", 1))
        return lax.psum_scatter(values, "cp", scatter_dimension=1, tiled=True)

    query_raw = project(tokens_low, w_query)
    key_raw = project(tokens_low, w_key)
    value_raw = project(tokens_low, w_value)
    squares = tp_sum_small(
        jnp.stack([jnp.sum(query_raw * query_raw, -1), jnp.sum(key_raw * key_raw, -1)])
    )
    query_rs = lax.rsqrt(squares[0] / model_width + EPS)[:, None]
    key_rs = lax.rsqrt(squares[1] / model_width + EPS)[:, None]
    query_norm = query_raw * query_rs * gain_query
    key_norm = key_raw * key_rs * gain_key
    query_low = (
        rope_turn(query_norm.reshape(row_count, head_count, HEAD_DIM), places, 1.0)
        .astype(jnp.bfloat16)
        .reshape(seq_count, shard_rows, local_width)
    )
    key_low = (
        rope_turn(key_norm.reshape(row_count, head_count, HEAD_DIM), places, 1.0)
        .astype(jnp.bfloat16)
        .reshape(seq_count, shard_rows, local_width)
    )
    value_low = value_raw.astype(jnp.bfloat16).reshape(seq_count, shard_rows, local_width)
    all_values = whole_sequence(value_low)
    all_keys = whole_sequence(key_low)
    token_split = Split(tokens_low, place, fast)

    def scores_for(query_seq, key_seq, segment_seq, code_seq):
        length = key_seq.shape[0]
        query_heads = query_seq.reshape(shard_rows, head_count, HEAD_DIM)
        key_heads = key_seq.reshape(length, head_count, HEAD_DIM)
        scores = (
            jnp.einsum("qhd,khd->hqk", query_heads, key_heads, preferred_element_type=jnp.float32)
            * score_scale
        )
        allowed = (key_index[None, :] <= query_index[:, None]) & (
            (code_seq[None, :] == segment_seq[:, None])
            | (key_index[None, :] == query_index[:, None])
        )
        return jnp.where(allowed[None], scores, NEG)

    def forward_seq(seq_items):
        query_seq, key_seq, value_seq, segment_seq, code_seq = seq_items
        length = key_seq.shape[0]
        scores = scores_for(query_seq, key_seq, segment_seq, code_seq)
        largest = jnp.max(scores, -1, keepdims=True)
        raw_weights = jnp.exp(scores - largest)
        totals = jnp.sum(raw_weights, -1, keepdims=True)
        probs_low = (raw_weights / totals).astype(jnp.bfloat16)
        value_heads = value_seq.reshape(length, head_count, HEAD_DIM)
        attended = jnp.einsum(
            "hqk,khd->qhd", probs_low, value_heads, preferred_element_type=jnp.float32
        )
        return (attended.reshape(shard_rows, local_width), (largest + jnp.log(totals))[..., 0])

    attended, log_totals = lax.map(
        forward_seq, (query_low, all_keys, all_values, source_ids, all_codes)
    )
    attn_low = local_order(attended.reshape(row_count, local_width).astype(jnp.bfloat16), core)
    attn_there = exchange(attn_low)
    tokens_local = local_order(tokens_low, core)
    upstream_local = local_order(cotangent.reshape(row_count, model_width), core)

    def chunk(values, number):
        return values[number * chunk_rows : (number + 1) * chunk_rows]

    outputs, hiddens, acts, grad_mlps, grad_gates, grad_ups = [], [], [], [], [], []
    grad_hiddens, grad_attns, grad_attendeds = [], [], []
    gain_sums = []
    kept = []
    for number in range(CHUNKS):
        branch_a = wide(tp_sum(project(chunk(attn_low, number), w_out)))
        attn_rs = lax.rsqrt(jnp.mean(branch_a * branch_a, -1, keepdims=True) + EPS)
        hidden = wide(chunk(tokens_local, number)) + branch_a * attn_rs * gain_attn
        hidden_low = hidden.astype(jnp.bfloat16)
        gate = project(hidden_low, w_gate)
        up_part = project(hidden_low, w_up)
        gate_sigmoid = jax.nn.sigmoid(gate)
        act_low = (gate * gate_sigmoid * up_part).astype(jnp.bfloat16)
        hiddens.append(hidden_low)
        acts.append(act_low)
        kept.append((branch_a, attn_rs, hidden, gate, up_part, gate_sigmoid))
    hidden_split = Split(jnp.concatenate(hiddens, 0), place, fast)
    act_low = jnp.concatenate(acts, 0)
    act_there = exchange(act_low)
    for number in range(CHUNKS):
        branch_a, attn_rs, hidden, gate, up_part, gate_sigmoid = kept[number]
        branch_m = wide(tp_sum(project(acts[number], w_down)))
        mlp_rs = lax.rsqrt(jnp.mean(branch_m * branch_m, -1, keepdims=True) + EPS)
        outputs.append((hidden + branch_m * mlp_rs * gain_mlp).astype(jnp.bfloat16))
        upstream = wide(chunk(upstream_local, number))
        inner = jnp.mean(branch_m * gain_mlp * upstream, -1, keepdims=True)
        grad_mlp_low = (
            mlp_rs * gain_mlp * upstream - branch_m * mlp_rs**3 * inner
        ).astype(jnp.bfloat16)
        mlp_gain_sum = jnp.sum((upstream * branch_m * mlp_rs)[:own_rows], 0)
        grad_act = project_back(grad_mlp_low, w_down)
        grad_up_low = (grad_act * gate * gate_sigmoid).astype(jnp.bfloat16)
        grad_gate_low = (
            grad_act * up_part * gate_sigmoid * (1.0 + gate * (1.0 - gate_sigmoid))
        ).astype(jnp.bfloat16)
        grad_mlps.append(grad_mlp_low)
        grad_ups.append(grad_up_low)
        grad_gates.append(grad_gate_low)
        grad_hidden = upstream + wide(
            tp_sum(project_back(grad_gate_low, w_gate) + project_back(grad_up_low, w_up))
        )
        inner = jnp.mean(branch_a * gain_attn * grad_hidden, -1, keepdims=True)
        grad_attn_low = (
            attn_rs * gain_attn * grad_hidden - branch_a * attn_rs**3 * inner
        ).astype(jnp.bfloat16)
        attn_gain_sum = jnp.sum((grad_hidden * branch_a * attn_rs)[:own_rows], 0)
        gain_sums.append(jnp.concatenate([attn_gain_sum, mlp_gain_sum]))
        grad_hiddens.append(grad_hidden)
        grad_attns.append(grad_attn_low)
        grad_attendeds.append(project_back(grad_attn_low, w_out).astype(jnp.bfloat16))
    output = local_order(jnp.concatenate(outputs, 0), core)
    mlp_split = Split(jnp.concatenate(grad_mlps, 0), place, fast)
    grad_w_down = split_grad(mlp_split, act_low, act_there, 1)
    grad_gate_low = jnp.concatenate(grad_gates, 0)
    grad_w_gate = split_grad(hidden_split, grad_gate_low, exchange(grad_gate_low), 0)
    grad_up_low = jnp.concatenate(grad_ups, 0)
    grad_w_up = split_grad(hidden_split, grad_up_low, exchange(grad_up_low), 0)
    attn_split = Split(jnp.concatenate(grad_attns, 0), place, fast)
    grad_w_out = split_grad(attn_split, attn_low, attn_there, 1)
    gain_sum = sum(gain_sums[1:], gain_sums[0])
    gain_sum = token_sum(gain_sum + swap(gain_sum, "tp", 1))
    grad_attended = local_order(jnp.concatenate(grad_attendeds, 0), core).reshape(
        seq_count, shard_rows, local_width
    )

    def backward_seq(seq_items):
        query_seq, key_seq, value_seq, segment_seq, code_seq, log_seq, grad_seq = seq_items
        length = key_seq.shape[0]
        scores = scores_for(query_seq, key_seq, segment_seq, code_seq)
        probs = jnp.exp(scores - log_seq[..., None])
        probs_low = probs.astype(jnp.bfloat16)
        query_heads = query_seq.reshape(shard_rows, head_count, HEAD_DIM)
        key_heads = key_seq.reshape(length, head_count, HEAD_DIM)
        value_heads = value_seq.reshape(length, head_count, HEAD_DIM)
        grad_heads = grad_seq.reshape(shard_rows, head_count, HEAD_DIM)
        grad_probs = jnp.einsum(
            "qhd,khd->hqk", grad_heads, value_heads, preferred_element_type=jnp.float32
        )
        grad_scores = (
            probs * (grad_probs - jnp.sum(probs * grad_probs, -1, keepdims=True))
        ).astype(jnp.bfloat16)
        grad_query = (
            jnp.einsum("hqk,khd->qhd", grad_scores, key_heads, preferred_element_type=jnp.float32)
            * score_scale
        )
        grad_key = (
            jnp.einsum("hqk,qhd->khd", grad_scores, query_heads, preferred_element_type=jnp.float32)
            * score_scale
        )
        grad_value = jnp.einsum(
            "hqk,qhd->khd", probs_low, grad_heads, preferred_element_type=jnp.float32
        )
        return (
            grad_query.reshape(shard_rows, local_width),
            grad_key.reshape(length, local_width),
            grad_value.reshape(length, local_width),
        )

    grad_qrot, grad_kall, grad_vall = lax.map(
        backward_seq,
        (query_low, all_keys, all_values, source_ids, all_codes, log_totals, grad_attended),
    )
    grad_value = back_to_block(grad_vall)
    grad_krot = back_to_block(grad_kall)
    grad_qnorm = rope_turn(
        grad_qrot.reshape(row_count, head_count, HEAD_DIM), places, -1.0
    ).reshape(row_count, local_width)
    grad_knorm = rope_turn(
        grad_krot.reshape(row_count, head_count, HEAD_DIM), places, -1.0
    ).reshape(row_count, local_width)
    inners = tp_sum_small(
        jnp.stack(
            [
                jnp.sum(query_raw * gain_query * grad_qnorm, -1),
                jnp.sum(key_raw * gain_key * grad_knorm, -1),
            ]
        )
    )
    qk_gain_sum = token_sum(
        jnp.concatenate(
            [
                jnp.sum(grad_qnorm * query_raw * query_rs, 0),
                jnp.sum(grad_knorm * key_raw * key_rs, 0),
            ]
        )
    )
    grad_qraw_low = (
        query_rs * gain_query * grad_qnorm
        - query_raw * query_rs**3 * (inners[0] / model_width)[:, None]
    ).astype(jnp.bfloat16)
    grad_kraw_low = (
        key_rs * gain_key * grad_knorm - key_raw * key_rs**3 * (inners[1] / model_width)[:, None]
    ).astype(jnp.bfloat16)
    grad_value_low = grad_value.reshape(row_count, local_width).astype(jnp.bfloat16)
    grads_low = jnp.concatenate([grad_qraw_low, grad_kraw_low, grad_value_low], 1)
    grads_there = exchange(grads_low)
    grads_local = local_order(grads_low, core)
    grad_rows = []
    for number in range(CHUNKS):
        rows = chunk(grads_local, number)
        input_terms = (
            project_back(rows[:, :local_width], w_query)
            + project_back(rows[:, local_width : 2 * local_width], w_key)
            + project_back(rows[:, 2 * local_width :], w_value)
        )
        grad_rows.append((grad_hiddens[number] + wide(tp_sum(input_terms))).astype(jnp.bfloat16))
    grad_tokens = local_order(jnp.concatenate(grad_rows, 0), core)
    grad_w_in = split_grad(token_split, grads_low, grads_there, 0)
    return (
        output.reshape(tokens.shape),
        grad_tokens.reshape(tokens.shape),
        grad_w_in[:, :local_width],
        grad_w_in[:, local_width : 2 * local_width],
        grad_w_in[:, 2 * local_width :],
        grad_w_out,
        grad_w_gate,
        grad_w_up,
        grad_w_down,
        qk_gain_sum[:local_width],
        qk_gain_sum[local_width:],
        gain_sum[:model_width],
        gain_sum[model_width:],
    )


def solution(mesh):
    return jax.shard_map(
        shards,
        mesh=mesh,
        in_specs=(
            P("dp", "cp", None),
            P("dp", "cp"),
            P("dp", "cp"),
            P("dp", "cp", None),
            P(None, "tp"),
            P(None, "tp"),
            P(None, "tp"),
            P("tp", None),
            P(None, "tp"),
            P(None, "tp"),
            P("tp", None),
            P("tp"),
            P("tp"),
            P(),
            P(),
        ),
        out_specs=(
            P("dp", "cp", None),
            P("dp", "cp", None),
            P(("dp", "cp"), "tp"),
            P(("dp", "cp"), "tp"),
            P(("dp", "cp"), "tp"),
            P("tp", ("dp", "cp")),
            P(("dp", "cp"), "tp"),
            P(("dp", "cp"), "tp"),
            P("tp", ("dp", "cp")),
            P("tp"),
            P("tp"),
            P(),
            P(),
        ),
        check_vma=False,
    )
```
